32 devices in a mesh: parts: 2 (over y), blk: 4 (over z), sub: 2 (over x), rep: 2 (over core).
Axes of the slice: x: 2, y: 2, z: 4, core: 2. Of those that a mesh axis runs over, the one named last changes fastest.
Arguments:
- queries: bfloat16 [128, 32, 128], P(('parts', 'blk', 'sub', 'rep')), parts along dimension 0, may hold values from -1.5 to 1.5
- passages: bfloat16 [512, 128, 128], P(('parts', 'blk')), parts along dimension 0, may hold values from -1.5 to 1.5
- lengths: int32 [512], P(('parts', 'blk')), parts along dimension 0, may hold values from 8 to 128
- slot_of: int32 [512], P('parts'), parts along dimension 0, may hold values from 0 to 255, each once
- candidates: int32 [128, 256], P(('parts', 'blk', 'sub', 'rep')), parts along dimension 0, may hold values from 0 to 255
Outputs:
- score: float32 [128, 256], P(('parts', 'blk', 'sub', 'rep')), parts along dimension 0
- top: float32 [128, 10], P(('parts', 'blk', 'sub', 'rep')), parts along dimension 0
The draws below stay inside these ranges and needn't reach their ends.
There are 2 independent parts, one for each index of `parts`. The reference program is written for one: setup_inputs(seed, part) draws one part's arguments, and reference() takes and returns one part's arrays. A program takes and returns all parts, laid end to end along the dimension named above; each array names one. Nothing has to cross between parts.
Inputs may be any that keep to these rules, and one draw needn't show every extreme that they name: `slot_of`: a permutation; storage row r lies on the blk index r // 64. `candidates`: passage ids, repeats allowed. `lengths`: the live slots of a row are its first ones.
All inputs are finite; a program needn't handle non-finite values.
Results may differ from the reference program's by a relative error of at most 0.0003.
Values may be sent and summed in bfloat16 or wider, within the bound.
A program may use at most 64 MiB of HBM per device.

```python
import math
import jax
import jax.numpy as jnp
import numpy as np
from jax import lax

DIM = 128
QT = 32
LP = 128
K = 256
TOPN = 10
NQ = 64
NP = 256


def set_ends(drawn, stream_key, low, high):
    extent = drawn.shape
    index_at = [jax.random.randint(jax.random.fold_in(stream_key, axis), (), 0, extent[axis]) for axis in range(len(extent))]
    drawn = drawn.at[tuple(index_at)].set(low)
    longest = extent.index(max(extent))
    index_at[longest] = (index_at[longest] + 1) % extent[longest]
    return drawn.at[tuple(index_at)].set(high)


def steps_of(own_key, extent, split, least, high):
    loudness, own = 1.0, jax.random.fold_in(own_key, 6)
    for axis_at, shards_of in split:
        heights = jnp.exp(jax.random.uniform(jax.random.fold_in(own, axis_at), (shards_of,), jnp.float32, least / len(split), high / len(split)))
        loudness = loudness * jnp.repeat(heights, extent[axis_at] // shards_of).reshape([-1 if axis == axis_at else 1 for axis in range(len(extent))])
    return loudness


def cumulative_ranks(count, skew):
    loads = [(1 << 20) // math.isqrt(grade ** skew) + 1 for grade in range(1, count + 1)]
    scale = 1 + sum(loads) // (1 << 30)
    return np.cumsum(np.array([max(1, weight // scale) for weight in loads]))


def skewed_ids(own_key, extent, number_of, lean):
    grid = cumulative_ranks(number_of, lean)
    ticket = jax.random.randint(jax.random.fold_in(own_key, 1), extent, 0, int(grid[number_of - 1]))
    grade = jnp.searchsorted(jnp.asarray(grid, jnp.int32), ticket, side="right")
    return jax.random.permutation(jax.random.fold_in(own_key, 2), number_of)[grade].astype(jnp.int32)


def noise(key, extent, scale, bound, pieces=(), kind=jnp.bfloat16):
    entries = jax.random.normal(key, extent, jnp.float32) * scale
    if len(pieces) > 0:
        entries = steps_of(key, extent, pieces, -0.22, 0.18) * entries
    return jnp.clip(entries, min=-bound, max=bound).astype(kind)


def setup_inputs(seed: int = 0, part: int = 0) -> dict:
    key_of = jax.random.split(jax.random.key(seed), 6)
    part_splits = jax.random.split(jax.random.fold_in(key_of[5], part), 6)
    return {
        "queries": noise(part_splits[0], (NQ, QT, DIM), 0.25, 1.5, ((0, 16),)),
        "passages": noise(part_splits[1], (NP, LP, DIM), 0.25, 1.5, ((0, 4),)),
        "lengths": set_ends(jax.random.randint(part_splits[2], (NP,), 8, LP + 1), jax.random.fold_in(part_splits[2], 1), 8, LP).astype(jnp.int32),
        "slot_of": jax.random.permutation(part_splits[3], NP).astype(jnp.int32),
        "candidates": set_ends(skewed_ids(part_splits[4], (NQ, K), NP, 2), jax.random.fold_in(part_splits[4], 3), 0, NP - 1).astype(jnp.int32),
    }


def reference(queries, passages, lengths, slot_of, candidates):
    query_count = queries.shape[0]
    passage_count = passages.shape[0]
    flat = queries.reshape(query_count * QT, DIM)
    blocks = passages.reshape(passage_count // 8, 8 * LP, DIM)
    spans = lengths.reshape(passage_count // 8, 8)

    def one_block(pair):
        piece, live_count = pair
        similar = jnp.dot(flat, piece.T, preferred_element_type=jnp.float32)
        similar = similar.reshape(query_count * QT, 8, LP)
        live = jnp.arange(LP, dtype=jnp.int32)[None, :] < live_count[:, None]
        best = jnp.max(jnp.where(live[None], similar, -1e30), axis=2)
        return jnp.sum(best.reshape(query_count, QT, 8), axis=1) / QT

    table = lax.map(one_block, (blocks, spans))
    table = jnp.transpose(table, (1, 0, 2)).reshape(query_count, passage_count)
    storage_rows = jnp.take(slot_of, candidates, axis=0).astype(jnp.int32)
    score = jnp.take_along_axis(table, storage_rows, axis=1)
    top = lax.top_k(score, TOPN)[0]
    return score, top
```

```python
import functools

import jax
import jax.numpy as jnp
from jax import lax
from jax.experimental import pallas as pl
from jax.experimental.pallas import tpu as pltpu
from jax.sharding import PartitionSpec as P

TOPN = 10
LANES = 128
ROWS = 8
MESH = pl.DeviceIdType.MESH


def lookup(tiles, width, index):
    tile_at, lane_at = index // width, index % width
    found = None
    for i, tile in enumerate(tiles):
        here = jnp.take_along_axis(tile, lane_at, axis=1, mode="promise_in_bounds")
        found = here if found is None else jnp.where(tile_at == i, here, found)
    return found


def kernel(n, lengths, slot_of, candidates, queries, passages, score_out, top_out,
           stored, asked, answer, replies, load_sem, query_sem, ask_send, ask_recv, reply_send, reply_recv):
    me = lax.axis_index("blk")
    count, span, width = passages.shape
    held, tokens, _ = queries.shape
    wide = held * tokens
    half = span // 2
    pieces = load_sem.shape[0]
    per_piece = count // pieces

    own_queries = pltpu.make_async_copy(queries, asked.at[0], query_sem)
    own_queries.start()
    loads = []
    for c in range(pieces):
        part = pl.ds(c * per_piece, per_piece)
        loads.append(pltpu.make_async_copy(passages.at[part], stored.at[part], load_sem.at[c]))
        loads[-1].start()

    barrier = pltpu.get_barrier_semaphore()
    for step in range(1, n):
        pl.semaphore_signal(barrier, inc=1, device_id={"blk": lax.rem(me + step, n)}, device_id_type=MESH)

    wanted = candidates[...]
    wanted = jnp.concatenate([wanted] * (ROWS // held), axis=0)
    ids = slot_of.shape[1]
    slots = [jnp.broadcast_to(slot_of[:, i:i + LANES], (ROWS, LANES)) for i in range(0, ids, LANES)]
    rows = [lookup(slots, LANES, wanted[:, i:i + LANES]) for i in range(0, wanted.shape[1], LANES)]

    own_queries.wait()
    pl.semaphore_wait(barrier, n - 1)
    asks = []
    for step in range(1, n):
        ask = pltpu.make_async_remote_copy(
            src_ref=asked.at[0], dst_ref=asked.at[step], send_sem=ask_send.at[step], recv_sem=ask_recv.at[step],
            device_id={"blk": lax.rem(me + step, n)}, device_id_type=MESH)
        ask.start()
        asks.append(ask)

    slot_at = lax.broadcasted_iota(jnp.int32, (span, width), 0)

    def fill(r, carry):
        piece = stored[r]
        first = jnp.broadcast_to(piece[0:1], (span, width))
        stored[r] = jnp.where(slot_at < lengths[r], piece, first)
        return carry

    for c in range(pieces):
        loads[c].wait()
        lax.fori_loop(c * per_piece, (c + 1) * per_piece, fill, 0, unroll=4)

    pick = lax.broadcasted_iota(jnp.int32, (ROWS, wide), 1) // tokens
    pick = jnp.where(pick == lax.broadcasted_iota(jnp.int32, (ROWS, wide), 0), 1.0 / tokens, 0.0).astype(jnp.bfloat16)
    group = 16

    def scores_of(source):
        flat = asked[source].reshape(wide, width)
        blank = jnp.zeros((wide, width), jnp.bfloat16)
        both = jnp.concatenate(
            [jnp.concatenate([flat, blank], axis=1), jnp.concatenate([blank, flat], axis=1)], axis=0)
        bests = []
        for g in range(0, count, group):
            piece = stored[g:g + group]
            pair = jnp.concatenate([piece[:, :half], piece[:, half:]], axis=2).reshape(group * half, 2 * width)
            similar = lax.dot_general(pair, both, (((1,), (1,)), ((), ())), preferred_element_type=jnp.float32)
            best = jnp.max(similar.reshape(group, half, 2 * wide), axis=1)
            bests.append(jnp.maximum(best[:, :wide], best[:, wide:]))
        best = jnp.concatenate(bests, axis=0)
        high = best.astype(jnp.bfloat16)
        low = (best - high.astype(jnp.float32)).astype(jnp.bfloat16)
        dims = (((1,), (1,)), ((), ()))
        return (lax.dot_general(pick, high, dims, preferred_element_type=jnp.float32)
                + lax.dot_general(pick, low, dims, preferred_element_type=jnp.float32))

    def put(ref, at, value):
        ref[at] = jnp.concatenate([value, jnp.zeros((ROWS, LANES - count), jnp.float32)], axis=1)

    put(replies, 0, scores_of(0))
    sends = []
    for step in range(1, n):
        asks[step - 1].wait_recv()
        put(answer, step, scores_of(step))
        back = pltpu.make_async_remote_copy(
            src_ref=answer.at[step], dst_ref=replies.at[step], send_sem=reply_send.at[step],
            recv_sem=reply_recv.at[step], device_id={"blk": lax.rem(me + n - step, n)}, device_id_type=MESH)
        back.start()
        sends.append(back)
    for send in sends:
        send.wait_recv()

    owners = [lax.rem(row // count + (n - me), n) * count + row % count for row in rows]
    tables = [replies[s] for s in range(n)]
    score = jnp.concatenate([lookup(tables, count, row) for row in owners], axis=1)
    score_out[...] = score[:held]

    total = score.shape[1]
    turned = jnp.transpose(score)
    earlier = lax.broadcasted_iota(jnp.int32, (total, total), 0) < lax.broadcasted_iota(jnp.int32, (total, total), 1)
    depth = top_out.shape[0]
    place = lax.broadcasted_iota(jnp.int32, (depth, total), 0).astype(jnp.float32)
    tops = jnp.zeros((depth, LANES), jnp.float32)
    lane = lax.broadcasted_iota(jnp.int32, (depth, LANES), 1)
    for q in range(held):
        here = score[q:q + 1]
        there = jnp.broadcast_to(turned[:, q:q + 1], (total, total))
        ahead = (there > here) | ((there == here) & earlier)
        rank = jnp.sum(jnp.where(ahead, 1.0, 0.0), axis=0, keepdims=True)
        chosen = jnp.sum(jnp.where(rank == place, here, 0.0), axis=1, keepdims=True)
        tops = jnp.where(lane == q, chosen, tops)
    top_out[...] = tops

    for copy in asks:
        copy.wait_send()
    for send in sends:
        send.wait_send()


def shards(n, queries, passages, lengths, slot_of, candidates):
    held, tokens, width = queries.shape
    depth = -(-TOPN // ROWS) * ROWS
    vmem = pl.BlockSpec(memory_space=pltpu.VMEM)
    hbm = pl.BlockSpec(memory_space=pl.ANY)
    score, top = pl.pallas_call(
        functools.partial(kernel, n),
        out_shape=(
            jax.ShapeDtypeStruct(candidates.shape, jnp.float32),
            jax.ShapeDtypeStruct((depth, LANES), jnp.float32),
        ),
        in_specs=[pl.BlockSpec(memory_space=pltpu.SMEM), vmem, vmem, hbm, hbm],
        out_specs=(vmem, vmem),
        scratch_shapes=[
            pltpu.VMEM(passages.shape, jnp.bfloat16),
            pltpu.VMEM((n, held, tokens, width), jnp.bfloat16),
            pltpu.VMEM((n, ROWS, LANES), jnp.float32),
            pltpu.VMEM((n, ROWS, LANES), jnp.float32),
            pltpu.SemaphoreType.DMA((4,)),
            pltpu.SemaphoreType.DMA,
            pltpu.SemaphoreType.DMA((n,)),
            pltpu.SemaphoreType.DMA((n,)),
            pltpu.SemaphoreType.DMA((n,)),
            pltpu.SemaphoreType.DMA((n,)),
        ],
        compiler_params=pltpu.CompilerParams(collective_id=0, has_side_effects=True),
    )(lengths, slot_of.reshape(1, -1), candidates, queries, passages)
    return score, jnp.transpose(top[:TOPN, :held])


def solution(mesh):
    return jax.shard_map(
        functools.partial(shards, mesh.shape["blk"]),
        mesh=mesh,
        in_specs=(
            P(("parts", "blk", "sub", "rep"), None, None),
            P(("parts", "blk"), None, None),
            P(("parts", "blk")),
            P("parts"),
            P(("parts", "blk", "sub", "rep"), None),
        ),
        out_specs=(
            P(("parts", "blk", "sub", "rep"), None),
            P(("parts", "blk", "sub", "rep"), None),
        ),
        check_vma=False,
    )
```

```python
import functools

import jax
import jax.numpy as jnp
from jax import lax
from jax.experimental import pallas as pl
from jax.experimental.pallas import tpu as pltpu
from jax.sharding import PartitionSpec as P

TOPN = 10
LANES = 128
ROWS = 8
MESH = pl.DeviceIdType.MESH


def split(index, width):
    if width & (width - 1):
        return lax.div(index, width), lax.rem(index, width)
    return lax.shift_right_logical(index, width.bit_length() - 1), index & (width - 1)


def lookup(tiles, places):
    tile_at, lane_at = places
    found = None
    for i, tile in enumerate(tiles):
        here = jnp.take_along_axis(tile, lane_at, axis=1, mode="promise_in_bounds")
        found = here if found is None else jnp.where(tile_at == i, here, found)
    return found


def peer_at(me, n, step):
    upper = lax.div(2 * me, n)
    room = me * (1 - upper) + (n - 1 - me) * upper
    inner = lax.div(step + 1, 2) * (1 - 2 * lax.rem(step + 1, 2))
    outer = (step - room) * (1 - 2 * upper)
    return me + jnp.where(step <= 2 * room, inner, outer)


def kernel(n, lengths_in, slot_in, wanted_in, queries, passages, score_out, top_out,
           stored, asked, answer, replies, lengths, slot_of, wanted_at,
           load_sem, small_sem, ask_send, ask_recv, reply_send, reply_recv):
    me = lax.axis_index("blk")
    count, span, width = passages.shape
    held, tokens, _ = queries.shape
    wide = held * tokens
    half = span // 2
    pieces = load_sem.shape[0]
    per_piece = count // pieces

    barrier = pltpu.get_barrier_semaphore()
    for step in range(1, n):
        pl.semaphore_signal(barrier, inc=1, device_id={"blk": lax.rem(me + step, n)}, device_id_type=MESH)

    smalls = []
    for i, (src, dst) in enumerate(((queries, asked.at[me]), (lengths_in, lengths), (slot_in, slot_of), (wanted_in, wanted_at))):
        smalls.append(pltpu.make_async_copy(src, dst, small_sem.at[i]))
        smalls[-1].start()
    loads = []
    for c in range(pieces):
        part = pl.ds(c * per_piece, per_piece)
        loads.append(pltpu.make_async_copy(passages.at[part], stored.at[part], load_sem.at[c]))
        loads[-1].start()

    def ask(step):
        peer = peer_at(me, n, step)
        return pltpu.make_async_remote_copy(
            src_ref=asked.at[me], dst_ref=asked.at[me], send_sem=ask_send.at[step], recv_sem=ask_recv.at[me],
            device_id={"blk": peer}, device_id_type=MESH)

    def asked_by(peer):
        return pltpu.make_async_remote_copy(
            src_ref=asked.at[me], dst_ref=asked.at[peer], send_sem=ask_send.at[0], recv_sem=ask_recv.at[peer],
            device_id={"blk": peer}, device_id_type=MESH)

    def reply(step):
        peer = peer_at(me, n, step)
        return pltpu.make_async_remote_copy(
            src_ref=answer.at[step], dst_ref=replies.at[me], send_sem=reply_send.at[step],
            recv_sem=reply_recv.at[me], device_id={"blk": peer}, device_id_type=MESH)

    def replied_by(peer):
        return pltpu.make_async_remote_copy(
            src_ref=answer.at[0], dst_ref=replies.at[peer], send_sem=reply_send.at[0],
            recv_sem=reply_recv.at[peer], device_id={"blk": peer}, device_id_type=MESH)

    smalls[0].wait()
    pl.semaphore_wait(barrier, n - 1)
    for step in range(1, n):
        ask(step).start()
    for small in smalls[1:]:
        small.wait()

    slot_at = lax.broadcasted_iota(jnp.int32, (span, width), 0)

    def fill(r, carry):
        piece = stored[r]
        first = jnp.broadcast_to(piece[0:1], (span, width))
        stored[r] = jnp.where(slot_at < lengths[r], piece, first)
        return carry

    for c in range(pieces):
        loads[c].wait()
        lax.fori_loop(c * per_piece, (c + 1) * per_piece, fill, 0, unroll=4)

    wanted = jnp.concatenate([wanted_at[...]] * (ROWS // held), axis=0)
    slots = [jnp.broadcast_to(slot_of[:, i:i + LANES], (ROWS, LANES)) for i in range(0, slot_of.shape[1], LANES)]
    rows = [lookup(slots, split(wanted[:, i:i + LANES], LANES)) for i in range(0, wanted.shape[1], LANES)]
    places = [split(row, count) for row in rows]

    pick = split(lax.broadcasted_iota(jnp.int32, (ROWS, wide), 1), tokens)[0]
    pick = jnp.where(pick == lax.broadcasted_iota(jnp.int32, (ROWS, wide), 0), 1.0 / tokens, 0.0).astype(jnp.bfloat16)
    group = 16

    def scores_of(source):
        flat = asked[source].reshape(wide, width)
        blank = jnp.zeros((wide, width), jnp.bfloat16)
        both = jnp.concatenate(
            [jnp.concatenate([flat, blank], axis=1), jnp.concatenate([blank, flat], axis=1)], axis=0)
        bests = []
        for g in range(0, count, group):
            piece = stored[g:g + group]
            pair = jnp.concatenate([piece[:, :half], piece[:, half:]], axis=2).reshape(group * half, 2 * width)
            similar = lax.dot_general(pair, both, (((1,), (1,)), ((), ())), preferred_element_type=jnp.float32)
            best = jnp.max(similar.reshape(group, half, 2 * wide), axis=1)
            bests.append(jnp.maximum(best[:, :wide], best[:, wide:]))
        best = jnp.concatenate(bests, axis=0)
        high = best.astype(jnp.bfloat16)
        low = (best - high.astype(jnp.float32)).astype(jnp.bfloat16)
        dims = (((1,), (1,)), ((), ()))
        table = (lax.dot_general(pick, high, dims, preferred_element_type=jnp.float32)
                 + lax.dot_general(pick, low, dims, preferred_element_type=jnp.float32))
        return jnp.concatenate([table, jnp.zeros((ROWS, LANES - count), jnp.float32)], axis=1)

    replies[me] = scores_of(me)

    def serve(step, carry):
        peer = peer_at(me, n, step)
        asked_by(peer).wait_recv()
        answer[step] = scores_of(peer)
        reply(step).start()
        return carry

    lax.fori_loop(1, n, serve, 0)

    for step in range(1, n):
        replied_by(peer_at(me, n, step)).wait_recv()

    tables = [replies[s] for s in range(n)]
    score = jnp.concatenate([lookup(tables, place) for place in places], axis=1)
    score_out[...] = score[:held]

    total = score.shape[1]
    turned = jnp.transpose(score)
    earlier = lax.broadcasted_iota(jnp.int32, (total, total), 0) < lax.broadcasted_iota(jnp.int32, (total, total), 1)
    depth = -(-TOPN // ROWS) * ROWS
    place = lax.broadcasted_iota(jnp.int32, (depth, total), 0).astype(jnp.float32)
    tops = jnp.zeros((depth, LANES), jnp.float32)
    lane = lax.broadcasted_iota(jnp.int32, (depth, LANES), 1)
    for q in range(held):
        here = score[q:q + 1]
        there = jnp.broadcast_to(turned[:, q:q + 1], (total, total))
        ahead = (there > here) | ((there == here) & earlier)
        rank = jnp.sum(jnp.where(ahead, 1.0, 0.0), axis=0, keepdims=True)
        chosen = jnp.sum(jnp.where(rank == place, here, 0.0), axis=1, keepdims=True)
        tops = jnp.where(lane == q, chosen, tops)
    top_out[...] = jnp.transpose(tops)[:held, :TOPN]

    for step in range(1, n):
        ask(step).wait_send()
        reply(step).wait_send()


def publish(score_in, top_in, score_out, top_out):
    score_out[...] = score_in[...]
    top_out[...] = top_in[...]


def shards(n, queries, passages, lengths, slot_of, candidates):
    held, tokens, width = queries.shape
    vmem = pl.BlockSpec(memory_space=pltpu.VMEM)
    hbm = pl.BlockSpec(memory_space=pl.ANY)
    slot_row = slot_of.reshape(1, -1)
    results = [(candidates.shape, jnp.float32), ((held, TOPN), jnp.float32)]
    score, top = pl.pallas_call(
        functools.partial(kernel, n),
        out_shape=tuple(pltpu.VMEM(shape, dtype) for shape, dtype in results),
        in_specs=[hbm] * 5,
        out_specs=(vmem, vmem),
        scratch_shapes=[
            pltpu.VMEM(passages.shape, jnp.bfloat16),
            pltpu.VMEM((n, held, tokens, width), jnp.bfloat16),
            pltpu.VMEM((n, ROWS, LANES), jnp.float32),
            pltpu.VMEM((n, ROWS, LANES), jnp.float32),
            pltpu.SMEM(lengths.shape, jnp.int32),
            pltpu.VMEM(slot_row.shape, jnp.int32),
            pltpu.VMEM(candidates.shape, jnp.int32),
            pltpu.SemaphoreType.DMA((4,)),
            pltpu.SemaphoreType.DMA((4,)),
            pltpu.SemaphoreType.DMA((n,)),
            pltpu.SemaphoreType.DMA((n,)),
            pltpu.SemaphoreType.DMA((n,)),
            pltpu.SemaphoreType.DMA((n,)),
        ],
        compiler_params=pltpu.CompilerParams(collective_id=0, has_side_effects=True),
    )(lengths, slot_row, candidates, queries, passages)
    return pl.pallas_call(
        publish,
        out_shape=tuple(jax.ShapeDtypeStruct(shape, dtype) for shape, dtype in results),
        in_specs=[vmem, vmem],
        compiler_params=pltpu.CompilerParams(vmem_limit_bytes=1 << 20),
        out_specs=(vmem, vmem),
    )(score, top)


def solution(mesh):
    return jax.shard_map(
        functools.partial(shards, mesh.shape["blk"]),
        mesh=mesh,
        in_specs=(
            P(("parts", "blk", "sub", "rep"), None, None),
            P(("parts", "blk"), None, None),
            P(("parts", "blk")),
            P("parts"),
            P(("parts", "blk", "sub", "rep"), None),
        ),
        out_specs=(
            P(("parts", "blk", "sub", "rep"), None),
            P(("parts", "blk", "sub", "rep"), None),
        ),
        check_vma=False,
    )
```

```python
import functools

import jax
import jax.numpy as jnp
from jax import lax
from jax.experimental import pallas as pl
from jax.experimental.pallas import tpu as pltpu
from jax.sharding import PartitionSpec as P

TOPN = 10
LANES = 128
ROWS = 8
MESH = pl.DeviceIdType.MESH


def split(index, width):
    if width & (width - 1):
        return lax.div(index, width), lax.rem(index, width)
    return lax.shift_right_logical(index, width.bit_length() - 1), index & (width - 1)


def lookup(tiles, places):
    tile_at, lane_at = places
    found = None
    for i, tile in enumerate(tiles):
        here = jnp.take_along_axis(tile, lane_at, axis=1, mode="promise_in_bounds")
        found = here if found is None else jnp.where(tile_at == i, here, found)
    return found


def peer_at(me, n, step):
    upper = lax.div(2 * me, n)
    room = me * (1 - upper) + (n - 1 - me) * upper
    inner = lax.div(step + 1, 2) * (1 - 2 * lax.rem(step + 1, 2))
    outer = (step - room) * (1 - 2 * upper)
    return me + jnp.where(step <= 2 * room, inner, outer)


def source_at(me, n, step):
    at = n - step
    return at - jnp.where(at <= me, 1, 0)


def kernel(n, copies, lengths_in, slot_in, wanted_in, queries, passages, score_out, top_out,
           stored, asked, answer, replies, lengths, slot_of, wanted_at,
           load_sem, small_sem, ask_send, ask_recv, reply_send, reply_recv):
    me = lax.axis_index("blk")
    other = copies - 1 - lax.axis_index("rep")
    count, span, width = passages.shape
    held, tokens, _ = queries.shape
    wide = held * tokens
    half = span // 2
    pieces = load_sem.shape[0]
    per_piece = count // pieces

    barrier = pltpu.get_barrier_semaphore()
    for step in range(1, n):
        pl.semaphore_signal(barrier, inc=1, device_id={"blk": lax.rem(me + step, n), "rep": other}, device_id_type=MESH)

    smalls = []
    for i, (src, dst) in enumerate(((queries, asked.at[me]), (lengths_in, lengths), (slot_in, slot_of), (wanted_in, wanted_at))):
        smalls.append(pltpu.make_async_copy(src, dst, small_sem.at[i]))
        smalls[-1].start()
    loads = []
    for c in range(pieces):
        part = pl.ds(c * per_piece, per_piece)
        loads.append(pltpu.make_async_copy(passages.at[part], stored.at[part], load_sem.at[c]))
        loads[-1].start()

    def ask(step):
        peer = peer_at(me, n, step)
        return pltpu.make_async_remote_copy(
            src_ref=asked.at[me], dst_ref=asked.at[me], send_sem=ask_send.at[step], recv_sem=ask_recv.at[me],
            device_id={"blk": peer, "rep": other}, device_id_type=MESH)

    def asked_by(peer):
        return pltpu.make_async_remote_copy(
            src_ref=asked.at[me], dst_ref=asked.at[peer], send_sem=ask_send.at[0], recv_sem=ask_recv.at[peer],
            device_id={"blk": peer, "rep": other}, device_id_type=MESH)

    def reply(step):
        peer = source_at(me, n, step)
        return pltpu.make_async_remote_copy(
            src_ref=answer.at[step], dst_ref=replies.at[me], send_sem=reply_send.at[step],
            recv_sem=reply_recv.at[me], device_id={"blk": peer, "rep": other}, device_id_type=MESH)

    def replied_by(peer):
        return pltpu.make_async_remote_copy(
            src_ref=answer.at[0], dst_ref=replies.at[peer], send_sem=reply_send.at[0],
            recv_sem=reply_recv.at[peer], device_id={"blk": peer, "rep": other}, device_id_type=MESH)

    smalls[0].wait()
    pl.semaphore_wait(barrier, n - 1)
    for step in range(n - 1, 0, -1):
        ask(step).start()
    for small in smalls[1:]:
        small.wait()

    slot_at = lax.broadcasted_iota(jnp.int32, (span, width), 0)

    def fill(r, carry):
        piece = stored[r]
        first = jnp.broadcast_to(piece[0:1], (span, width))
        stored[r] = jnp.where(slot_at < lengths[r], piece, first)
        return carry

    for c in range(pieces):
        loads[c].wait()
        lax.fori_loop(c * per_piece, (c + 1) * per_piece, fill, 0, unroll=4)

    wanted = jnp.concatenate([wanted_at[...]] * (ROWS // held), axis=0)
    slots = [jnp.broadcast_to(slot_of[:, i:i + LANES], (ROWS, LANES)) for i in range(0, slot_of.shape[1], LANES)]
    rows = [lookup(slots, split(wanted[:, i:i + LANES], LANES)) for i in range(0, wanted.shape[1], LANES)]
    places = [split(row, count) for row in rows]

    pick = split(lax.broadcasted_iota(jnp.int32, (ROWS, wide), 1), tokens)[0]
    pick = jnp.where(pick == lax.broadcasted_iota(jnp.int32, (ROWS, wide), 0), 1.0 / tokens, 0.0).astype(jnp.bfloat16)
    group = 16

    def scores_of(source):
        flat = asked[source].reshape(wide, width)
        blank = jnp.zeros((wide, width), jnp.bfloat16)
        both = jnp.concatenate(
            [jnp.concatenate([flat, blank], axis=1), jnp.concatenate([blank, flat], axis=1)], axis=0)
        bests = []
        for g in range(0, count, group):
            piece = stored[g:g + group]
            pair = jnp.concatenate([piece[:, :half], piece[:, half:]], axis=2).reshape(group * half, 2 * width)
            similar = lax.dot_general(pair, both, (((1,), (1,)), ((), ())), preferred_element_type=jnp.float32)
            best = jnp.max(similar.reshape(group, half, 2 * wide), axis=1)
            bests.append(jnp.maximum(best[:, :wide], best[:, wide:]))
        best = jnp.concatenate(bests, axis=0)
        high = best.astype(jnp.bfloat16)
        low = (best - high.astype(jnp.float32)).astype(jnp.bfloat16)
        dims = (((1,), (1,)), ((), ()))
        table = (lax.dot_general(pick, high, dims, preferred_element_type=jnp.float32)
                 + lax.dot_general(pick, low, dims, preferred_element_type=jnp.float32))
        return jnp.concatenate([table, jnp.zeros((ROWS, LANES - count), jnp.float32)], axis=1)

    replies[me] = scores_of(me)

    def serve(step, carry):
        peer = source_at(me, n, step)
        asked_by(peer).wait_recv()
        answer[step] = scores_of(peer)
        reply(step).start()
        return carry

    lax.fori_loop(1, n, serve, 0)

    for step in range(1, n):
        replied_by(peer_at(me, n, step)).wait_recv()

    tables = [replies[s] for s in range(n)]
    score = jnp.concatenate([lookup(tables, place) for place in places], axis=1)
    score_out[...] = score[:held]

    total = score.shape[1]
    turned = jnp.transpose(score)
    earlier = lax.broadcasted_iota(jnp.int32, (total, total), 0) < lax.broadcasted_iota(jnp.int32, (total, total), 1)
    depth = -(-TOPN // ROWS) * ROWS
    place = lax.broadcasted_iota(jnp.int32, (depth, total), 0).astype(jnp.float32)
    tops = jnp.zeros((depth, LANES), jnp.float32)
    lane = lax.broadcasted_iota(jnp.int32, (depth, LANES), 1)
    for q in range(held):
        here = score[q:q + 1]
        there = jnp.broadcast_to(turned[:, q:q + 1], (total, total))
        ahead = (there > here) | ((there == here) & earlier)
        rank = jnp.sum(jnp.where(ahead, 1.0, 0.0), axis=0, keepdims=True)
        chosen = jnp.sum(jnp.where(rank == place, here, 0.0), axis=1, keepdims=True)
        tops = jnp.where(lane == q, chosen, tops)
    top_out[...] = jnp.transpose(tops)[:held, :TOPN]

    for step in range(1, n):
        ask(step).wait_send()
        reply(step).wait_send()


def publish(score_in, top_in, score_out, top_out):
    score_out[...] = score_in[...]
    top_out[...] = top_in[...]


def shards(n, copies, queries, passages, lengths, slot_of, candidates):
    held, tokens, width = queries.shape
    vmem = pl.BlockSpec(memory_space=pltpu.VMEM)
    hbm = pl.BlockSpec(memory_space=pl.ANY)
    slot_row = slot_of.reshape(1, -1)
    results = [(candidates.shape, jnp.float32), ((held, TOPN), jnp.float32)]
    score, top = pl.pallas_call(
        functools.partial(kernel, n, copies),
        out_shape=tuple(pltpu.VMEM(shape, dtype) for shape, dtype in results),
        in_specs=[hbm] * 5,
        out_specs=(vmem, vmem),
        scratch_shapes=[
            pltpu.VMEM(passages.shape, jnp.bfloat16),
            pltpu.VMEM((n, held, tokens, width), jnp.bfloat16),
            pltpu.VMEM((n, ROWS, LANES), jnp.float32),
            pltpu.VMEM((n, ROWS, LANES), jnp.float32),
            pltpu.SMEM(lengths.shape, jnp.int32),
            pltpu.VMEM(slot_row.shape, jnp.int32),
            pltpu.VMEM(candidates.shape, jnp.int32),
            pltpu.SemaphoreType.DMA((4,)),
            pltpu.SemaphoreType.DMA((4,)),
            pltpu.SemaphoreType.DMA((n,)),
            pltpu.SemaphoreType.DMA((n,)),
            pltpu.SemaphoreType.DMA((n,)),
            pltpu.SemaphoreType.DMA((n,)),
        ],
        compiler_params=pltpu.CompilerParams(collective_id=0, has_side_effects=True),
    )(lengths, slot_row, candidates, queries, passages)
    return pl.pallas_call(
        publish,
        out_shape=tuple(jax.ShapeDtypeStruct(shape, dtype) for shape, dtype in results),
        in_specs=[vmem, vmem],
        compiler_params=pltpu.CompilerParams(vmem_limit_bytes=1 << 20),
        out_specs=(vmem, vmem),
    )(score, top)


def solution(mesh):
    return jax.shard_map(
        functools.partial(shards, mesh.shape["blk"], mesh.shape["rep"]),
        mesh=mesh,
        in_specs=(
            P(("parts", "blk", "sub", "rep"), None, None),
            P(("parts", "blk"), None, None),
            P(("parts", "blk")),
            P("parts"),
            P(("parts", "blk", "sub", "rep"), None),
        ),
        out_specs=(
            P(("parts", "blk", "sub", "rep"), None),
            P(("parts", "blk", "sub", "rep"), None),
        ),
        check_vma=False,
    )
```

```python
import functools

import jax
import jax.numpy as jnp
from jax import lax
from jax.experimental import pallas as pl
from jax.experimental.pallas import tpu as pltpu
from jax.sharding import PartitionSpec as P

TOPN = 10
LANES = 128
ROWS = 8
MESH = pl.DeviceIdType.MESH


def split(index, width):
    if width & (width - 1):
        return lax.div(index, width), lax.rem(index, width)
    return lax.shift_right_logical(index, width.bit_length() - 1), index & (width - 1)


def lookup(tiles, places):
    tile_at, lane_at = places
    found = None
    for i, tile in enumerate(tiles):
        here = jnp.take_along_axis(tile, lane_at, axis=1, mode="promise_in_bounds")
        found = here if found is None else jnp.where(tile_at == i, here, found)
    return found


def peer_at(me, n, step):
    upper = lax.div(2 * me, n)
    room = me * (1 - upper) + (n - 1 - me) * upper
    inner = lax.div(step + 1, 2) * (1 - 2 * lax.rem(step + 1, 2))
    outer = (step - room) * (1 - 2 * upper)
    return me + jnp.where(step <= 2 * room, inner, outer)


def source_at(me, n, step):
    at = n - step
    return at - jnp.where(at <= me, 1, 0)


def kernel(n, copies, lengths_in, slot_in, wanted_in, queries, passages, score_out, top_out,
           stored, asked, answer, replies, lengths, slot_of, wanted_at,
           load_sem, small_sem, ask_send, ask_recv, reply_send, reply_recv):
    me = lax.axis_index("blk")
    other = copies - 1 - lax.axis_index("rep")
    count, span, width = passages.shape
    held, tokens, _ = queries.shape
    wide = held * tokens
    half = span // 2
    pieces = load_sem.shape[0]
    per_piece = count // pieces

    barrier = pltpu.get_barrier_semaphore()
    for step in range(1, n):
        pl.semaphore_signal(barrier, inc=1, device_id={"blk": lax.rem(me + step, n), "rep": other}, device_id_type=MESH)

    smalls = []
    for i, (src, dst) in enumerate(((queries, asked.at[me]), (lengths_in, lengths), (slot_in, slot_of), (wanted_in, wanted_at))):
        smalls.append(pltpu.make_async_copy(src, dst, small_sem.at[i]))
        smalls[-1].start()
    loads = []
    for c in range(pieces):
        part = pl.ds(c * per_piece, per_piece)
        loads.append(pltpu.make_async_copy(passages.at[part], stored.at[part], load_sem.at[c]))
        loads[-1].start()

    def ask(step):
        peer = peer_at(me, n, step)
        return pltpu.make_async_remote_copy(
            src_ref=asked.at[me], dst_ref=asked.at[me], send_sem=ask_send.at[step], recv_sem=ask_recv.at[me],
            device_id={"blk": peer, "rep": other}, device_id_type=MESH)

    def asked_by(peer):
        return pltpu.make_async_remote_copy(
            src_ref=asked.at[me], dst_ref=asked.at[peer], send_sem=ask_send.at[0], recv_sem=ask_recv.at[peer],
            device_id={"blk": peer, "rep": other}, device_id_type=MESH)

    def reply(step):
        peer = source_at(me, n, step)
        return pltpu.make_async_remote_copy(
            src_ref=answer.at[step], dst_ref=replies.at[me], send_sem=reply_send.at[step],
            recv_sem=reply_recv.at[me], device_id={"blk": peer, "rep": other}, device_id_type=MESH)

    def replied_by(peer):
        return pltpu.make_async_remote_copy(
            src_ref=answer.at[0], dst_ref=replies.at[peer], send_sem=reply_send.at[0],
            recv_sem=reply_recv.at[peer], device_id={"blk": peer, "rep": other}, device_id_type=MESH)

    smalls[0].wait()
    pl.semaphore_wait(barrier, n - 1)
    for step in range(n - 1, 0, -1):
        ask(step).start()
    for small in smalls[1:]:
        small.wait()

    slot_at = lax.broadcasted_iota(jnp.int32, (span, width), 0)

    def fill(r, carry):
        piece = stored[r]
        first = jnp.broadcast_to(piece[0:1], (span, width))
        stored[r] = jnp.where(slot_at < lengths[r], piece, first)
        return carry

    for c in range(pieces):
        loads[c].wait()
        lax.fori_loop(c * per_piece, (c + 1) * per_piece, fill, 0, unroll=4)

    wanted = jnp.concatenate([wanted_at[...]] * (ROWS // held), axis=0)
    slots = [jnp.broadcast_to(slot_of[:, i:i + LANES], (ROWS, LANES)) for i in range(0, slot_of.shape[1], LANES)]
    rows = [lookup(slots, split(wanted[:, i:i + LANES], LANES)) for i in range(0, wanted.shape[1], LANES)]
    places = [split(row, count) for row in rows]

    pick = split(lax.broadcasted_iota(jnp.int32, (ROWS, wide), 1), tokens)[0]
    pick = jnp.where(pick == lax.broadcasted_iota(jnp.int32, (ROWS, wide), 0), 1.0 / tokens, 0.0).astype(jnp.bfloat16)
    group = 16

    def scores_of(source):
        flat = asked[source].reshape(wide, width)
        blank = jnp.zeros((wide, width), jnp.bfloat16)
        both = jnp.concatenate(
            [jnp.concatenate([flat, blank], axis=1), jnp.concatenate([blank, flat], axis=1)], axis=0)
        bests = []
        for g in range(0, count, group):
            piece = stored[g:g + group]
            pair = jnp.concatenate([piece[:, :half], piece[:, half:]], axis=2).reshape(group * half, 2 * width)
            similar = lax.dot_general(pair, both, (((1,), (1,)), ((), ())), preferred_element_type=jnp.float32)
            best = jnp.max(similar.reshape(group, half, 2 * wide), axis=1)
            bests.append(jnp.maximum(best[:, :wide], best[:, wide:]))
        best = jnp.concatenate(bests, axis=0)
        high = best.astype(jnp.bfloat16)
        low = (best - high.astype(jnp.float32)).astype(jnp.bfloat16)
        dims = (((1,), (1,)), ((), ()))
        table = (lax.dot_general(pick, high, dims, preferred_element_type=jnp.float32)
                 + lax.dot_general(pick, low, dims, preferred_element_type=jnp.float32))
        return jnp.concatenate([table, jnp.zeros((ROWS, LANES - count), jnp.float32)], axis=1)

    replies[me] = scores_of(me)

    def serve(step, carry):
        peer = source_at(me, n, step)
        asked_by(peer).wait_recv()
        answer[step] = scores_of(peer)
        reply(step).start()
        return carry

    lax.fori_loop(1, n, serve, 0)

    def from_owner(owner, score):
        table = replies[owner]
        return [jnp.where(tile_at == owner, jnp.take_along_axis(table, lane_at, axis=1, mode="promise_in_bounds"), found)
                for (tile_at, lane_at), found in zip(places, score)]

    score = from_owner(me, [jnp.zeros((ROWS, LANES), jnp.float32)] * len(places))
    for step in range(1, n):
        owner = peer_at(me, n, step)
        replied_by(owner).wait_recv()
        score = from_owner(owner, score)
    score = jnp.concatenate(score, axis=1)
    score_out[...] = score[:held]

    total = score.shape[1]
    turned = jnp.transpose(score)
    depth = -(-TOPN // ROWS) * ROWS
    place = lax.broadcasted_iota(jnp.int32, (depth, total), 0).astype(jnp.float32)
    tops = jnp.zeros((depth, LANES), jnp.float32)
    lane = lax.broadcasted_iota(jnp.int32, (depth, LANES), 1)
    for q in range(held):
        here = score[q:q + 1]
        there = jnp.broadcast_to(turned[:, q:q + 1], (total, total))
        larger = jnp.sum(jnp.where(there > here, 1.0, 0.0), axis=0, keepdims=True)
        chosen = jnp.min(jnp.where(larger <= place, here, jnp.inf), axis=1, keepdims=True)
        tops = jnp.where(lane == q, chosen, tops)
    top_out[...] = jnp.transpose(tops)[:held, :TOPN]

    for step in range(1, n):
        ask(step).wait_send()
        reply(step).wait_send()


def publish(score_in, top_in, score_out, top_out):
    score_out[...] = score_in[...]
    top_out[...] = top_in[...]


def shards(n, copies, queries, passages, lengths, slot_of, candidates):
    held, tokens, width = queries.shape
    vmem = pl.BlockSpec(memory_space=pltpu.VMEM)
    hbm = pl.BlockSpec(memory_space=pl.ANY)
    slot_row = slot_of.reshape(1, -1)
    results = [(candidates.shape, jnp.float32), ((held, TOPN), jnp.float32)]
    score, top = pl.pallas_call(
        functools.partial(kernel, n, copies),
        out_shape=tuple(pltpu.VMEM(shape, dtype) for shape, dtype in results),
        in_specs=[hbm] * 5,
        out_specs=(vmem, vmem),
        scratch_shapes=[
            pltpu.VMEM(passages.shape, jnp.bfloat16),
            pltpu.VMEM((n, held, tokens, width), jnp.bfloat16),
            pltpu.VMEM((n, ROWS, LANES), jnp.float32),
            pltpu.VMEM((n, ROWS, LANES), jnp.float32),
            pltpu.SMEM(lengths.shape, jnp.int32),
            pltpu.VMEM(slot_row.shape, jnp.int32),
            pltpu.VMEM(candidates.shape, jnp.int32),
            pltpu.SemaphoreType.DMA((4,)),
            pltpu.SemaphoreType.DMA((4,)),
            pltpu.SemaphoreType.DMA((n,)),
            pltpu.SemaphoreType.DMA((n,)),
            pltpu.SemaphoreType.DMA((n,)),
            pltpu.SemaphoreType.DMA((n,)),
        ],
        compiler_params=pltpu.CompilerParams(collective_id=0, has_side_effects=True),
    )(lengths, slot_row, candidates, queries, passages)
    return pl.pallas_call(
        publish,
        out_shape=tuple(jax.ShapeDtypeStruct(shape, dtype) for shape, dtype in results),
        in_specs=[vmem, vmem],
        compiler_params=pltpu.CompilerParams(vmem_limit_bytes=1 << 20),
        out_specs=(vmem, vmem),
    )(score, top)


def solution(mesh):
    return jax.shard_map(
        functools.partial(shards, mesh.shape["blk"], mesh.shape["rep"]),
        mesh=mesh,
        in_specs=(
            P(("parts", "blk", "sub", "rep"), None, None),
            P(("parts", "blk"), None, None),
            P(("parts", "blk")),
            P("parts"),
            P(("parts", "blk", "sub", "rep"), None),
        ),
        out_specs=(
            P(("parts", "blk", "sub", "rep"), None),
            P(("parts", "blk", "sub", "rep"), None),
        ),
        check_vma=False,
    )
```

```python
import functools

import jax
import jax.numpy as jnp
from jax import lax
from jax.experimental import pallas as pl
from jax.experimental.pallas import tpu as pltpu
from jax.sharding import PartitionSpec as P

TOPN = 10
LANES = 128
ROWS = 8
MESH = pl.DeviceIdType.MESH


def split(index, width):
    if width & (width - 1):
        return lax.div(index, width), lax.rem(index, width)
    return lax.shift_right_logical(index, width.bit_length() - 1), index & (width - 1)


def lookup(tiles, places):
    tile_at, lane_at = places
    found = None
    for i, tile in enumerate(tiles):
        here = jnp.take_along_axis(tile, lane_at, axis=1, mode="promise_in_bounds")
        found = here if found is None else jnp.where(tile_at == i, here, found)
    return found


def peer_at(me, n, step):
    upper = lax.div(2 * me, n)
    room = me * (1 - upper) + (n - 1 - me) * upper
    inner = lax.div(step + 1, 2) * (1 - 2 * lax.rem(step + 1, 2))
    outer = (step - room) * (1 - 2 * upper)
    return me + jnp.where(step <= 2 * room, inner, outer)


def source_at(me, n, step):
    at = step - 1
    return at + jnp.where(at >= me, 1, 0)


def kernel(n, copies, lengths_in, slot_in, wanted_in, queries, passages, score_out, top_out,
           stored, asked, answer, replies, lengths, slot_of, wanted_at,
           load_sem, small_sem, ask_send, ask_recv, reply_send, reply_recv):
    me = lax.axis_index("blk")
    other = copies - 1 - lax.axis_index("rep")
    count, span, width = passages.shape
    held, tokens, _ = queries.shape
    wide = held * tokens
    half = span // 2
    pieces = load_sem.shape[0]
    per_piece = count // pieces

    barrier = pltpu.get_barrier_semaphore()
    for step in range(1, n):
        pl.semaphore_signal(barrier, inc=1, device_id={"blk": lax.rem(me + step, n), "rep": other}, device_id_type=MESH)

    smalls = []
    for i, (src, dst) in enumerate(((queries, asked.at[me]), (lengths_in, lengths), (slot_in, slot_of), (wanted_in, wanted_at))):
        smalls.append(pltpu.make_async_copy(src, dst, small_sem.at[i]))
        smalls[-1].start()
    loads = []
    for c in range(pieces):
        part = pl.ds(c * per_piece, per_piece)
        loads.append(pltpu.make_async_copy(passages.at[part], stored.at[part], load_sem.at[c]))
        loads[-1].start()

    def ask(step):
        peer = peer_at(me, n, step)
        return pltpu.make_async_remote_copy(
            src_ref=asked.at[me], dst_ref=asked.at[me], send_sem=ask_send.at[step], recv_sem=ask_recv.at[me],
            device_id={"blk": peer, "rep": other}, device_id_type=MESH)

    def asked_by(peer):
        return pltpu.make_async_remote_copy(
            src_ref=asked.at[me], dst_ref=asked.at[peer], send_sem=ask_send.at[0], recv_sem=ask_recv.at[peer],
            device_id={"blk": peer, "rep": other}, device_id_type=MESH)

    def reply(step):
        peer = source_at(me, n, step)
        return pltpu.make_async_remote_copy(
            src_ref=answer.at[step], dst_ref=replies.at[me], send_sem=reply_send.at[step],
            recv_sem=reply_recv.at[me], device_id={"blk": peer, "rep": other}, device_id_type=MESH)

    def replied_by(peer):
        return pltpu.make_async_remote_copy(
            src_ref=answer.at[0], dst_ref=replies.at[peer], send_sem=reply_send.at[0],
            recv_sem=reply_recv.at[peer], device_id={"blk": peer, "rep": other}, device_id_type=MESH)

    smalls[0].wait()
    pl.semaphore_wait(barrier, n - 1)
    for step in range(n - 1, 0, -1):
        ask(step).start()
    for small in smalls[1:]:
        small.wait()

    slot_at = lax.broadcasted_iota(jnp.int32, (span, width), 0)

    def fill(r, carry):
        piece = stored[r]
        first = jnp.broadcast_to(piece[0:1], (span, width))
        stored[r] = jnp.where(slot_at < lengths[r], piece, first)
        return carry

    for c in range(pieces):
        loads[c].wait()
        lax.fori_loop(c * per_piece, (c + 1) * per_piece, fill, 0, unroll=4)

    wanted = jnp.concatenate([wanted_at[...]] * (ROWS // held), axis=0)
    slots = [jnp.broadcast_to(slot_of[:, i:i + LANES], (ROWS, LANES)) for i in range(0, slot_of.shape[1], LANES)]
    rows = [lookup(slots, split(wanted[:, i:i + LANES], LANES)) for i in range(0, wanted.shape[1], LANES)]
    places = [split(row, count) for row in rows]

    pick = split(lax.broadcasted_iota(jnp.int32, (ROWS, wide), 1), tokens)[0]
    pick = jnp.where(pick == lax.broadcasted_iota(jnp.int32, (ROWS, wide), 0), 1.0 / tokens, 0.0).astype(jnp.bfloat16)
    group = 16

    def scores_of(source):
        flat = asked[source].reshape(wide, width)
        blank = jnp.zeros((wide, width), jnp.bfloat16)
        both = jnp.concatenate(
            [jnp.concatenate([flat, blank], axis=1), jnp.concatenate([blank, flat], axis=1)], axis=0)
        bests = []
        for g in range(0, count, group):
            piece = stored[g:g + group]
            pair = jnp.concatenate([piece[:, :half], piece[:, half:]], axis=2).reshape(group * half, 2 * width)
            similar = lax.dot_general(pair, both, (((1,), (1,)), ((), ())), preferred_element_type=jnp.float32)
            best = jnp.max(similar.reshape(group, half, 2 * wide), axis=1)
            bests.append(jnp.maximum(best[:, :wide], best[:, wide:]))
        best = jnp.concatenate(bests, axis=0)
        high = best.astype(jnp.bfloat16)
        low = (best - high.astype(jnp.float32)).astype(jnp.bfloat16)
        dims = (((1,), (1,)), ((), ()))
        table = (lax.dot_general(pick, high, dims, preferred_element_type=jnp.float32)
                 + lax.dot_general(pick, low, dims, preferred_element_type=jnp.float32))
        return jnp.concatenate([table, jnp.zeros((ROWS, LANES - count), jnp.float32)], axis=1)

    replies[me] = scores_of(me)

    def serve(step, carry):
        peer = source_at(me, n, step)
        asked_by(peer).wait_recv()
        answer[step] = scores_of(peer)
        reply(step).start()
        return carry

    lax.fori_loop(1, n, serve, 0)

    def from_owner(owner, score):
        table = replies[owner]
        return [jnp.where(tile_at == owner, jnp.take_along_axis(table, lane_at, axis=1, mode="promise_in_bounds"), found)
                for (tile_at, lane_at), found in zip(places, score)]

    score = from_owner(me, [jnp.zeros((ROWS, LANES), jnp.float32)] * len(places))
    for step in range(1, n):
        owner = peer_at(me, n, step)
        replied_by(owner).wait_recv()
        score = from_owner(owner, score)
    score = jnp.concatenate(score, axis=1)
    score_out[...] = score[:held]

    total = score.shape[1]
    turned = jnp.transpose(score)
    depth = -(-TOPN // ROWS) * ROWS
    place = lax.broadcasted_iota(jnp.int32, (depth, total), 0).astype(jnp.float32)
    tops = jnp.zeros((depth, LANES), jnp.float32)
    lane = lax.broadcasted_iota(jnp.int32, (depth, LANES), 1)
    for q in range(held):
        here = score[q:q + 1]
        there = jnp.broadcast_to(turned[:, q:q + 1], (total, total))
        larger = jnp.sum(jnp.where(there > here, 1.0, 0.0), axis=0, keepdims=True)
        chosen = jnp.min(jnp.where(larger <= place, here, jnp.inf), axis=1, keepdims=True)
        tops = jnp.where(lane == q, chosen, tops)
    top_out[...] = jnp.transpose(tops)[:held, :TOPN]

    for step in range(1, n):
        ask(step).wait_send()
        reply(step).wait_send()


def publish(score_in, top_in, score_out, top_out):
    score_out[...] = score_in[...]
    top_out[...] = top_in[...]


def shards(n, copies, queries, passages, lengths, slot_of, candidates):
    held, tokens, width = queries.shape
    vmem = pl.BlockSpec(memory_space=pltpu.VMEM)
    hbm = pl.BlockSpec(memory_space=pl.ANY)
    slot_row = slot_of.reshape(1, -1)
    results = [(candidates.shape, jnp.float32), ((held, TOPN), jnp.float32)]
    score, top = pl.pallas_call(
        functools.partial(kernel, n, copies),
        out_shape=tuple(pltpu.VMEM(shape, dtype) for shape, dtype in results),
        in_specs=[hbm] * 5,
        out_specs=(vmem, vmem),
        scratch_shapes=[
            pltpu.VMEM(passages.shape, jnp.bfloat16),
            pltpu.VMEM((n, held, tokens, width), jnp.bfloat16),
            pltpu.VMEM((n, ROWS, LANES), jnp.float32),
            pltpu.VMEM((n, ROWS, LANES), jnp.float32),
            pltpu.SMEM(lengths.shape, jnp.int32),
            pltpu.VMEM(slot_row.shape, jnp.int32),
            pltpu.VMEM(candidates.shape, jnp.int32),
            pltpu.SemaphoreType.DMA((4,)),
            pltpu.SemaphoreType.DMA((4,)),
            pltpu.SemaphoreType.DMA((n,)),
            pltpu.SemaphoreType.DMA((n,)),
            pltpu.SemaphoreType.DMA((n,)),
            pltpu.SemaphoreType.DMA((n,)),
        ],
        compiler_params=pltpu.CompilerParams(collective_id=0, has_side_effects=True),
    )(lengths, slot_row, candidates, queries, passages)
    return pl.pallas_call(
        publish,
        out_shape=tuple(jax.ShapeDtypeStruct(shape, dtype) for shape, dtype in results),
        in_specs=[vmem, vmem],
        compiler_params=pltpu.CompilerParams(vmem_limit_bytes=1 << 20),
        out_specs=(vmem, vmem),
    )(score, top)


def solution(mesh):
    return jax.shard_map(
        functools.partial(shards, mesh.shape["blk"], mesh.shape["rep"]),
        mesh=mesh,
        in_specs=(
            P(("parts", "blk", "sub", "rep"), None, None),
            P(("parts", "blk"), None, None),
            P(("parts", "blk")),
            P("parts"),
            P(("parts", "blk", "sub", "rep"), None),
        ),
        out_specs=(
            P(("parts", "blk", "sub", "rep"), None),
            P(("parts", "blk", "sub", "rep"), None),
        ),
        check_vma=False,
    )
```

```python
import functools

import jax
import jax.numpy as jnp
from jax import lax
from jax.experimental import pallas as pl
from jax.experimental.pallas import tpu as pltpu
from jax.sharding import PartitionSpec as P

TOPN = 10
LANES = 128
ROWS = 8
MESH = pl.DeviceIdType.MESH


def split(index, width):
    if width & (width - 1):
        return lax.div(index, width), lax.rem(index, width)
    return lax.shift_right_logical(index, width.bit_length() - 1), index & (width - 1)


def lookup(tiles, places):
    tile_at, lane_at = places
    found = None
    for i, tile in enumerate(tiles):
        here = jnp.take_along_axis(tile, lane_at, axis=1, mode="promise_in_bounds")
        found = here if found is None else jnp.where(tile_at == i, here, found)
    return found


def peer_at(me, n, step):
    upper = lax.div(2 * me, n)
    room = me * (1 - upper) + (n - 1 - me) * upper
    inner = lax.div(step + 1, 2) * (1 - 2 * lax.rem(step + 1, 2))
    outer = (step - room) * (1 - 2 * upper)
    return me + jnp.where(step <= 2 * room, inner, outer)


def source_at(me, n, step):
    at = step - 1
    return at + jnp.where(at >= me, 1, 0)


def kernel(n, copies, lengths_in, slot_in, wanted_in, queries, passages, score_out, top_out,
           stored, asked, answer, replies, lengths, slot_of, wanted_at,
           load_sem, small_sem, ask_send, ask_recv, reply_send, reply_recv):
    me = lax.axis_index("blk")
    other = copies - 1 - lax.axis_index("rep")
    count, span, width = passages.shape
    held, tokens, _ = queries.shape
    wide = held * tokens
    half = span // 2
    pieces = load_sem.shape[0]
    per_piece = count // pieces

    barrier = pltpu.get_barrier_semaphore()
    for step in range(1, n):
        pl.semaphore_signal(barrier, inc=1, device_id={"blk": lax.rem(me + step, n), "rep": other}, device_id_type=MESH)

    smalls = []
    for i, (src, dst) in enumerate(((queries, asked.at[me]), (lengths_in, lengths), (slot_in, slot_of), (wanted_in, wanted_at))):
        smalls.append(pltpu.make_async_copy(src, dst, small_sem.at[i]))
        smalls[-1].start()
    loads = []
    for c in range(pieces):
        part = pl.ds(c * per_piece, per_piece)
        loads.append(pltpu.make_async_copy(passages.at[part], stored.at[part], load_sem.at[c]))
        loads[-1].start()

    def ask(step):
        peer = peer_at(me, n, step)
        return pltpu.make_async_remote_copy(
            src_ref=asked.at[me], dst_ref=asked.at[me], send_sem=ask_send.at[step], recv_sem=ask_recv.at[me],
            device_id={"blk": peer, "rep": other}, device_id_type=MESH)

    def asked_by(peer):
        return pltpu.make_async_remote_copy(
            src_ref=asked.at[me], dst_ref=asked.at[peer], send_sem=ask_send.at[0], recv_sem=ask_recv.at[peer],
            device_id={"blk": peer, "rep": other}, device_id_type=MESH)

    def reply(step):
        peer = source_at(me, n, step)
        return pltpu.make_async_remote_copy(
            src_ref=answer.at[step], dst_ref=replies.at[me], send_sem=reply_send.at[step],
            recv_sem=reply_recv.at[me], device_id={"blk": peer, "rep": other}, device_id_type=MESH)

    def replied_by(peer):
        return pltpu.make_async_remote_copy(
            src_ref=answer.at[0], dst_ref=replies.at[peer], send_sem=reply_send.at[0],
            recv_sem=reply_recv.at[peer], device_id={"blk": peer, "rep": other}, device_id_type=MESH)

    smalls[0].wait()
    pl.semaphore_wait(barrier, n - 1)
    for step in range(n - 1, 0, -1):
        ask(step).start()
    for small in smalls[1:]:
        small.wait()

    slot_at = lax.broadcasted_iota(jnp.int32, (span, width), 0)

    def fill(r, carry):
        piece = stored[r]
        first = jnp.broadcast_to(piece[0:1], (span, width))
        stored[r] = jnp.where(slot_at < lengths[r], piece, first)
        return carry

    for c in range(pieces):
        loads[c].wait()
        lax.fori_loop(c * per_piece, (c + 1) * per_piece, fill, 0, unroll=4)

    wanted = jnp.concatenate([wanted_at[...]] * (ROWS // held), axis=0)
    slots = [jnp.broadcast_to(slot_of[:, i:i + LANES], (ROWS, LANES)) for i in range(0, slot_of.shape[1], LANES)]
    rows = [lookup(slots, split(wanted[:, i:i + LANES], LANES)) for i in range(0, wanted.shape[1], LANES)]
    places = [split(row, count) for row in rows]

    pick = split(lax.broadcasted_iota(jnp.int32, (ROWS, wide), 1), tokens)[0]
    pick = jnp.where(pick == lax.broadcasted_iota(jnp.int32, (ROWS, wide), 0), 1.0 / tokens, 0.0).astype(jnp.bfloat16)
    pick = jnp.concatenate([pick, pick], axis=1)
    group = 4

    def scores_of(source):
        flat = asked[source].reshape(wide, width)
        blank = jnp.zeros((wide, width), jnp.bfloat16)
        both = jnp.concatenate(
            [jnp.concatenate([flat, blank], axis=1), jnp.concatenate([blank, flat], axis=1)], axis=0)
        bests = []
        for g in range(0, count, group):
            piece = stored[g:g + group]
            pair = jnp.concatenate([piece[:, :half], piece[:, half:]], axis=2).reshape(group * half, 2 * width)
            similar = lax.dot_general(pair, both, (((1,), (1,)), ((), ())), preferred_element_type=jnp.float32)
            best = jnp.max(similar.reshape(group, half, 2 * wide), axis=1)
            bests.append(jnp.maximum(best[:, :wide], best[:, wide:]))
        best = jnp.concatenate(bests, axis=0)
        high = best.astype(jnp.bfloat16)
        low = (best - high.astype(jnp.float32)).astype(jnp.bfloat16)
        halves = jnp.concatenate([high, low], axis=1)
        table = lax.dot_general(pick, halves, (((1,), (1,)), ((), ())), preferred_element_type=jnp.float32)
        return jnp.concatenate([table, jnp.zeros((ROWS, LANES - count), jnp.float32)], axis=1)

    replies[me] = scores_of(me)

    def serve(step, carry):
        peer = source_at(me, n, step)
        asked_by(peer).wait_recv()
        answer[step] = scores_of(peer)
        reply(step).start()
        return carry

    lax.fori_loop(1, n, serve, 0)

    def from_owner(owner, score):
        table = replies[owner]
        return [jnp.where(tile_at == owner, jnp.take_along_axis(table, lane_at, axis=1, mode="promise_in_bounds"), found)
                for (tile_at, lane_at), found in zip(places, score)]

    score = from_owner(me, [jnp.zeros((ROWS, LANES), jnp.float32)] * len(places))
    for step in range(1, n):
        owner = peer_at(me, n, step)
        replied_by(owner).wait_recv()
        score = from_owner(owner, score)
    score = jnp.concatenate(score, axis=1)
    score_out[...] = score[:held]

    total = score.shape[1]
    turned = jnp.transpose(score)
    depth = -(-TOPN // ROWS) * ROWS
    place = lax.broadcasted_iota(jnp.int32, (depth, total), 0).astype(jnp.float32)
    tops = jnp.zeros((depth, LANES), jnp.float32)
    lane = lax.broadcasted_iota(jnp.int32, (depth, LANES), 1)
    for q in range(held):
        here = score[q:q + 1]
        larger = jnp.zeros((ROWS, total), jnp.float32)
        for k in range(0, total, ROWS):
            there = jnp.broadcast_to(turned[k:k + ROWS, q:q + 1], (ROWS, total))
            larger = jnp.where(there > here, larger + 1.0, larger)
        larger = jnp.sum(larger, axis=0, keepdims=True)
        chosen = jnp.min(jnp.where(larger <= place, here, jnp.inf), axis=1, keepdims=True)
        tops = jnp.where(lane == q, chosen, tops)
    top_out[...] = jnp.transpose(tops)[:held, :TOPN]

    for step in range(1, n):
        ask(step).wait_send()
        reply(step).wait_send()


def publish(score_in, top_in, score_out, top_out):
    score_out[...] = score_in[...]
    top_out[...] = top_in[...]


def shards(n, copies, queries, passages, lengths, slot_of, candidates):
    held, tokens, width = queries.shape
    vmem = pl.BlockSpec(memory_space=pltpu.VMEM)
    hbm = pl.BlockSpec(memory_space=pl.ANY)
    slot_row = slot_of.reshape(1, -1)
    results = [(candidates.shape, jnp.float32), ((held, TOPN), jnp.float32)]
    score, top = pl.pallas_call(
        functools.partial(kernel, n, copies),
        out_shape=tuple(pltpu.VMEM(shape, dtype) for shape, dtype in results),
        in_specs=[hbm] * 5,
        out_specs=(vmem, vmem),
        scratch_shapes=[
            pltpu.VMEM(passages.shape, jnp.bfloat16),
            pltpu.VMEM((n, held, tokens, width), jnp.bfloat16),
            pltpu.VMEM((n, ROWS, LANES), jnp.float32),
            pltpu.VMEM((n, ROWS, LANES), jnp.float32),
            pltpu.SMEM(lengths.shape, jnp.int32),
            pltpu.VMEM(slot_row.shape, jnp.int32),
            pltpu.VMEM(candidates.shape, jnp.int32),
            pltpu.SemaphoreType.DMA((4,)),
            pltpu.SemaphoreType.DMA((4,)),
            pltpu.SemaphoreType.DMA((n,)),
            pltpu.SemaphoreType.DMA((n,)),
            pltpu.SemaphoreType.DMA((n,)),
            pltpu.SemaphoreType.DMA((n,)),
        ],
        compiler_params=pltpu.CompilerParams(collective_id=0, has_side_effects=True),
    )(lengths, slot_row, candidates, queries, passages)
    return pl.pallas_call(
        publish,
        out_shape=tuple(jax.ShapeDtypeStruct(shape, dtype) for shape, dtype in results),
        in_specs=[vmem, vmem],
        compiler_params=pltpu.CompilerParams(vmem_limit_bytes=1 << 20),
        out_specs=(vmem, vmem),
    )(score, top)


def solution(mesh):
    return jax.shard_map(
        functools.partial(shards, mesh.shape["blk"], mesh.shape["rep"]),
        mesh=mesh,
        in_specs=(
            P(("parts", "blk", "sub", "rep"), None, None),
            P(("parts", "blk"), None, None),
            P(("parts", "blk")),
            P("parts"),
            P(("parts", "blk", "sub", "rep"), None),
        ),
        out_specs=(
            P(("parts", "blk", "sub", "rep"), None),
            P(("parts", "blk", "sub", "rep"), None),
        ),
        check_vma=False,
    )
```

```python
import functools

import jax
import jax.numpy as jnp
from jax import lax
from jax.experimental import pallas as pl
from jax.experimental.pallas import tpu as pltpu
from jax.sharding import PartitionSpec as P

TOPN = 10
LANES = 128
ROWS = 8
MESH = pl.DeviceIdType.MESH


def split(index, width):
    if width & (width - 1):
        return lax.div(index, width), lax.rem(index, width)
    return lax.shift_right_logical(index, width.bit_length() - 1), index & (width - 1)


def lookup(tiles, places):
    tile_at, lane_at = places
    found = None
    for i, tile in enumerate(tiles):
        here = jnp.take_along_axis(tile, lane_at, axis=1, mode="promise_in_bounds")
        found = here if found is None else jnp.where(tile_at == i, here, found)
    return found


def peer_at(me, n, step):
    upper = lax.div(2 * me, n)
    room = me * (1 - upper) + (n - 1 - me) * upper
    inner = lax.div(step + 1, 2) * (1 - 2 * lax.rem(step + 1, 2))
    outer = (step - room) * (1 - 2 * upper)
    return me + jnp.where(step <= 2 * room, inner, outer)


def source_at(me, n, step):
    at = step - 1
    return at + jnp.where(at >= me, 1, 0)


def kernel(n, copies, lengths_in, slot_in, wanted_in, queries, passages, score_out, top_out,
           stored, asked, answer, replies, lengths, slot_of, wanted_at,
           load_sem, small_sem, ask_send, ask_recv, reply_send, reply_recv):
    me = lax.axis_index("blk")
    other = copies - 1 - lax.axis_index("rep")
    count, span, width = passages.shape
    held, tokens, _ = queries.shape
    wide = held * tokens
    half = span // 2
    pieces = load_sem.shape[0]
    per_piece = count // pieces

    barrier = pltpu.get_barrier_semaphore()
    for step in range(1, n):
        pl.semaphore_signal(barrier, inc=1, device_id={"blk": lax.rem(me + step, n), "rep": other}, device_id_type=MESH)

    smalls = []
    for i, (src, dst) in enumerate(((queries, asked.at[me]), (lengths_in, lengths), (slot_in, slot_of), (wanted_in, wanted_at))):
        smalls.append(pltpu.make_async_copy(src, dst, small_sem.at[i]))
        smalls[-1].start()
    loads = []
    for c in range(pieces):
        part = pl.ds(c * per_piece, per_piece)
        loads.append(pltpu.make_async_copy(passages.at[part], stored.at[part], load_sem.at[c]))
        loads[-1].start()

    def ask(step):
        peer = source_at(me, n, step)
        return pltpu.make_async_remote_copy(
            src_ref=asked.at[me], dst_ref=asked.at[me], send_sem=ask_send.at[step], recv_sem=ask_recv.at[me],
            device_id={"blk": peer, "rep": other}, device_id_type=MESH)

    def asked_by(peer):
        return pltpu.make_async_remote_copy(
            src_ref=asked.at[me], dst_ref=asked.at[peer], send_sem=ask_send.at[0], recv_sem=ask_recv.at[peer],
            device_id={"blk": peer, "rep": other}, device_id_type=MESH)

    def reply(step):
        peer = source_at(me, n, step)
        return pltpu.make_async_remote_copy(
            src_ref=answer.at[step], dst_ref=replies.at[me], send_sem=reply_send.at[step],
            recv_sem=reply_recv.at[me], device_id={"blk": peer, "rep": other}, device_id_type=MESH)

    def replied_by(peer):
        return pltpu.make_async_remote_copy(
            src_ref=answer.at[0], dst_ref=replies.at[peer], send_sem=reply_send.at[0],
            recv_sem=reply_recv.at[peer], device_id={"blk": peer, "rep": other}, device_id_type=MESH)

    smalls[0].wait()
    pl.semaphore_wait(barrier, n - 1)
    for step in range(n - 1, 0, -1):
        ask(step).start()
    for small in smalls[1:]:
        small.wait()

    slot_at = lax.broadcasted_iota(jnp.int32, (span, width), 0)

    def fill(r, carry):
        piece = stored[r]
        first = jnp.broadcast_to(piece[0:1], (span, width))
        stored[r] = jnp.where(slot_at < lengths[r], piece, first)
        return carry

    for c in range(pieces):
        loads[c].wait()
        lax.fori_loop(c * per_piece, (c + 1) * per_piece, fill, 0, unroll=4)

    wanted = jnp.concatenate([wanted_at[...]] * (ROWS // held), axis=0)
    slots = [jnp.broadcast_to(slot_of[:, i:i + LANES], (ROWS, LANES)) for i in range(0, slot_of.shape[1], LANES)]
    rows = [lookup(slots, split(wanted[:, i:i + LANES], LANES)) for i in range(0, wanted.shape[1], LANES)]
    places = [split(row, count) for row in rows]

    pick = split(lax.broadcasted_iota(jnp.int32, (ROWS, wide), 1), tokens)[0]
    pick = jnp.where(pick == lax.broadcasted_iota(jnp.int32, (ROWS, wide), 0), 1.0 / tokens, 0.0).astype(jnp.bfloat16)
    pick = jnp.concatenate([pick, pick], axis=1)
    group = 4

    def scores_of(source):
        flat = asked[source].reshape(wide, width)
        blank = jnp.zeros((wide, width), jnp.bfloat16)
        both = jnp.concatenate(
            [jnp.concatenate([flat, blank], axis=1), jnp.concatenate([blank, flat], axis=1)], axis=0)
        bests = []
        for g in range(0, count, group):
            piece = stored[g:g + group]
            pair = jnp.concatenate([piece[:, :half], piece[:, half:]], axis=2).reshape(group * half, 2 * width)
            similar = lax.dot_general(pair, both, (((1,), (1,)), ((), ())), preferred_element_type=jnp.float32)
            best = jnp.max(similar.reshape(group, half, 2 * wide), axis=1)
            bests.append(jnp.maximum(best[:, :wide], best[:, wide:]))
        best = jnp.concatenate(bests, axis=0)
        high = best.astype(jnp.bfloat16)
        low = (best - high.astype(jnp.float32)).astype(jnp.bfloat16)
        halves = jnp.concatenate([high, low], axis=1)
        table = lax.dot_general(pick, halves, (((1,), (1,)), ((), ())), preferred_element_type=jnp.float32)
        return jnp.concatenate([table, jnp.zeros((ROWS, LANES - count), jnp.float32)], axis=1)

    replies[me] = scores_of(me)

    def serve(step, carry):
        peer = source_at(me, n, step)
        asked_by(peer).wait_recv()
        answer[step] = scores_of(peer)
        reply(step).start()
        return carry

    lax.fori_loop(1, n, serve, 0)

    def from_owner(owner, score):
        table = replies[owner]
        return [jnp.where(tile_at == owner, jnp.take_along_axis(table, lane_at, axis=1, mode="promise_in_bounds"), found)
                for (tile_at, lane_at), found in zip(places, score)]

    score = from_owner(me, [jnp.zeros((ROWS, LANES), jnp.float32)] * len(places))
    for step in range(1, n):
        owner = peer_at(me, n, step)
        replied_by(owner).wait_recv()
        score = from_owner(owner, score)
    score = jnp.concatenate(score, axis=1)
    score_out[...] = score[:held]

    total = score.shape[1]
    turned = jnp.transpose(score)
    depth = -(-TOPN // ROWS) * ROWS
    place = lax.broadcasted_iota(jnp.int32, (depth, total), 0).astype(jnp.float32)
    tops = jnp.zeros((depth, LANES), jnp.float32)
    lane = lax.broadcasted_iota(jnp.int32, (depth, LANES), 1)
    for q in range(held):
        here = score[q:q + 1]
        larger = jnp.zeros((ROWS, total), jnp.float32)
        for k in range(0, total, ROWS):
            there = jnp.broadcast_to(turned[k:k + ROWS, q:q + 1], (ROWS, total))
            larger = jnp.where(there > here, larger + 1.0, larger)
        larger = jnp.sum(larger, axis=0, keepdims=True)
        chosen = jnp.min(jnp.where(larger <= place, here, jnp.inf), axis=1, keepdims=True)
        tops = jnp.where(lane == q, chosen, tops)
    top_out[...] = jnp.transpose(tops)[:held, :TOPN]

    for step in range(1, n):
        ask(step).wait_send()
        reply(step).wait_send()


def publish(score_in, top_in, score_out, top_out):
    score_out[...] = score_in[...]
    top_out[...] = top_in[...]


def shards(n, copies, queries, passages, lengths, slot_of, candidates):
    held, tokens, width = queries.shape
    vmem = pl.BlockSpec(memory_space=pltpu.VMEM)
    hbm = pl.BlockSpec(memory_space=pl.ANY)
    slot_row = slot_of.reshape(1, -1)
    results = [(candidates.shape, jnp.float32), ((held, TOPN), jnp.float32)]
    score, top = pl.pallas_call(
        functools.partial(kernel, n, copies),
        out_shape=tuple(pltpu.VMEM(shape, dtype) for shape, dtype in results),
        in_specs=[hbm] * 5,
        out_specs=(vmem, vmem),
        scratch_shapes=[
            pltpu.VMEM(passages.shape, jnp.bfloat16),
            pltpu.VMEM((n, held, tokens, width), jnp.bfloat16),
            pltpu.VMEM((n, ROWS, LANES), jnp.float32),
            pltpu.VMEM((n, ROWS, LANES), jnp.float32),
            pltpu.SMEM(lengths.shape, jnp.int32),
            pltpu.VMEM(slot_row.shape, jnp.int32),
            pltpu.VMEM(candidates.shape, jnp.int32),
            pltpu.SemaphoreType.DMA((4,)),
            pltpu.SemaphoreType.DMA((4,)),
            pltpu.SemaphoreType.DMA((n,)),
            pltpu.SemaphoreType.DMA((n,)),
            pltpu.SemaphoreType.DMA((n,)),
            pltpu.SemaphoreType.DMA((n,)),
        ],
        compiler_params=pltpu.CompilerParams(collective_id=0, has_side_effects=True),
    )(lengths, slot_row, candidates, queries, passages)
    return pl.pallas_call(
        publish,
        out_shape=tuple(jax.ShapeDtypeStruct(shape, dtype) for shape, dtype in results),
        in_specs=[vmem, vmem],
        compiler_params=pltpu.CompilerParams(vmem_limit_bytes=1 << 20),
        out_specs=(vmem, vmem),
    )(score, top)


def solution(mesh):
    return jax.shard_map(
        functools.partial(shards, mesh.shape["blk"], mesh.shape["rep"]),
        mesh=mesh,
        in_specs=(
            P(("parts", "blk", "sub", "rep"), None, None),
            P(("parts", "blk"), None, None),
            P(("parts", "blk")),
            P("parts"),
            P(("parts", "blk", "sub", "rep"), None),
        ),
        out_specs=(
            P(("parts", "blk", "sub", "rep"), None),
            P(("parts", "blk", "sub", "rep"), None),
        ),
        check_vma=False,
    )
```
